32 devices in a mesh: level: 4 (over z), dev: 8 (over y, x, core).
Axes of the slice: x: 2, y: 2, z: 4, core: 2. Of those that a mesh axis runs over, the one named last changes fastest.
Arguments:
- fields: float32 [4, 128, 12, 128], P('level', 'dev'), may hold values from -6 to 6
- own_src: int32 [4, 128], P('level', 'dev'), may hold values from 0 to 15
- own_weight: bfloat16 [4, 128, 128, 128], P('level', 'dev'), may hold values from 0 to 1, as said below
- send_block: int32 [4, 8, 8, 2], P('level', 'dev'), may hold values from 0 to 15
- send_target: int32 [4, 8, 8, 2], P('level', 'dev'), may hold values from 0 to 15
- send_count: int32 [4, 8, 8], P('level', 'dev'), may hold values from 0 to 2, as said below
- send_weight: bfloat16 [4, 8, 8, 2, 128, 128], P('level', 'dev'), may hold values from 0 to 1, as said below
- left_block: int32 [4, 8, 4, 2], P('level', 'dev'), may hold values from 0 to 15
- left_target: int32 [4, 8, 4, 2], P('level', 'dev'), may hold values from 0 to 15
- left_count: int32 [4, 8, 4], P('level', 'dev'), may hold values from 0 to 2, as said below
- left_weight: bfloat16 [4, 8, 4, 2, 128, 128], P('level', 'dev'), may hold values from 0 to 1, as said below
Outputs:
- remapped: float32 [4, 128, 12, 128], P('level', 'dev')
- totals: float32 [12], replicated
The draws below stay inside these ranges and needn't reach their ends.
Inputs may be any that keep to these rules, and one draw needn't show every extreme that they name: send_count[l, s, s] = 0; for every level some receiver device gets 2 live slots from every other device of the level. left_count[m, q, m] = 0; for every device index some receiver level gets 2 live slots from every other level. `own_weight`: nonnegative; entry [k, i] is zero where old cell k and new cell i differ by more than 3; each column sums to a positive intersect fraction of at most 1. `send_weight`: nonnegative; entry [k, i] is zero where old cell k and new cell i differ by more than 3; each column sums to a positive intersect fraction of at most 1. `left_weight`: nonnegative; entry [k, i] is zero where old cell k and new cell i differ by more than 3; each column sums to a positive intersect fraction of at most 1.
All inputs are finite; a program needn't handle non-finite values.
Results may differ from the reference program's by a relative error of at most 0.0045.
Values may be sent and summed in bfloat16 or wider, within the bound.
A program may use at most 64 MiB of HBM per device.

```python
import jax
import jax.numpy as jnp
from jax import lax

COMP = 12
CELLS = 128
HALF = 3
BLK_DEV = 16
CAP = 2
LCAP = 2
PEERS = 8
LEVELS = 4
BLOCKS = 128


def band_fractions(key, lead):
    first, second, third = jax.random.split(key, 3)
    shape = lead + (CELLS, CELLS)
    rowpos = lax.broadcasted_iota(jnp.int32, shape, len(lead))
    colpos = lax.broadcasted_iota(jnp.int32, shape, len(lead) + 1)
    spread = jnp.abs(rowpos - colpos)
    middle = jax.random.uniform(first, shape, jnp.float32, 2.0, 3.0)
    beside = jax.random.uniform(second, shape, jnp.float32, 0.3, 1.0)
    raw = jnp.where(spread == 0, middle, jnp.where(spread <= HALF, beside, jnp.zeros_like(beside)))
    fraction = jax.random.uniform(third, lead + (1, CELLS), jnp.float32, 0.2, 0.8)
    return raw / jnp.sum(raw, axis=-2, keepdims=True) * fraction


def draw_own_weight(key, part):
    whole = band_fractions(jax.random.fold_in(key, 11), (LEVELS, BLOCKS))
    return whole.astype(jnp.bfloat16)


def draw_send_weight(key, part):
    whole = band_fractions(jax.random.fold_in(key, 23), (LEVELS, PEERS, PEERS, CAP))
    return whole.astype(jnp.bfloat16)


def draw_left_weight(key, part):
    whole = band_fractions(jax.random.fold_in(key, 37), (LEVELS, PEERS, LEVELS, LCAP))
    return whole.astype(jnp.bfloat16)


def draw_send_count(key, part):
    shape = (LEVELS, PEERS, PEERS)
    base = jax.random.randint(key, shape, 0, CAP + 1)
    lvl = lax.broadcasted_iota(jnp.int32, shape, 0)
    src = lax.broadcasted_iota(jnp.int32, shape, 1)
    dst = lax.broadcasted_iota(jnp.int32, shape, 2)
    heavy = (7 * lvl + 3) % PEERS
    near = ((dst - src) % PEERS == 1) | ((src - dst) % PEERS == 1)
    full = (dst == heavy) | near
    out = jnp.where(full, CAP, base)
    return jnp.where(src == dst, 0, out).astype(jnp.int32)


def draw_left_count(key, part):
    shape = (LEVELS, PEERS, LEVELS)
    base = jax.random.randint(key, shape, 0, LCAP + 1)
    src = lax.broadcasted_iota(jnp.int32, shape, 0)
    dev = lax.broadcasted_iota(jnp.int32, shape, 1)
    dst = lax.broadcasted_iota(jnp.int32, shape, 2)
    heavy = (5 * dev + 1) % LEVELS
    near = ((dst - src) % LEVELS == 1) | ((src - dst) % LEVELS == 1)
    full = (dst == heavy) | near
    out = jnp.where(full, LCAP, base)
    return jnp.where(src == dst, 0, out).astype(jnp.int32)


def with_ends(drawn, own_key, smallest, top_value):
    spot = [jax.random.randint(jax.random.fold_in(own_key, axis), (), 0, length) for axis, length in enumerate(drawn.shape)]
    widest = drawn.shape.index(max(drawn.shape))
    next_to = spot[:widest] + [(spot[widest] + 1) % drawn.shape[widest]] + spot[widest + 1:]
    return drawn.at[tuple(spot)].set(smallest).at[tuple(next_to)].set(top_value)


def block_levels(key, shape, cuts, smallest, top_value):
    def one(position, parts):
        steps = jax.random.uniform(jax.random.fold_in(jax.random.fold_in(key, 6), position), (parts,), jnp.float32, smallest / len(cuts), top_value / len(cuts))
        return jnp.repeat(jnp.exp(steps), shape[position] // parts).reshape((-1,) + (1,) * (len(shape) - position - 1))

    loudness = one(*cuts[0])
    for cut in cuts[1:]:
        loudness = loudness * one(*cut)
    return loudness


def centred(rng, dims, deviation, reach, cuts=(), dtype=jnp.bfloat16):
    result = deviation * jax.random.normal(rng, dims, jnp.float32)
    if cuts:
        result = result * block_levels(rng, dims, cuts, -0.22, 0.18)
    return jnp.clip(result, -reach, reach).astype(dtype)


def setup_inputs(seed: int = 0) -> dict:
    splits = jax.random.split(jax.random.key(seed), 12)
    fields = centred(splits[0], (LEVELS, BLOCKS, COMP, CELLS), 1.0, 6.0, ((0, 4), (1, 8)), jnp.float32)
    own_src = with_ends(jax.random.randint(splits[1], (LEVELS, BLOCKS), 0, BLK_DEV), jax.random.fold_in(splits[1], 1), 0, BLK_DEV - 1).astype(jnp.int32)
    own_weight = draw_own_weight(jax.random.fold_in(splits[11], 71), 0)
    send_block = with_ends(jax.random.randint(splits[3], (LEVELS, PEERS, PEERS, CAP), 0, BLK_DEV), jax.random.fold_in(splits[3], 1), 0, BLK_DEV - 1).astype(jnp.int32)
    send_target = with_ends(jax.random.randint(splits[4], (LEVELS, PEERS, PEERS, CAP), 0, BLK_DEV), jax.random.fold_in(splits[4], 1), 0, BLK_DEV - 1).astype(jnp.int32)
    send_count = draw_send_count(jax.random.fold_in(splits[11], 71), 0)
    send_weight = draw_send_weight(jax.random.fold_in(splits[11], 71), 0)
    left_block = with_ends(jax.random.randint(splits[7], (LEVELS, PEERS, LEVELS, LCAP), 0, BLK_DEV), jax.random.fold_in(splits[7], 1), 0, BLK_DEV - 1).astype(jnp.int32)
    left_target = with_ends(jax.random.randint(splits[8], (LEVELS, PEERS, LEVELS, LCAP), 0, BLK_DEV), jax.random.fold_in(splits[8], 1), 0, BLK_DEV - 1).astype(jnp.int32)
    left_count = draw_left_count(jax.random.fold_in(splits[11], 71), 0)
    left_weight = draw_left_weight(jax.random.fold_in(splits[11], 71), 0)
    return dict(fields=fields, own_src=own_src, own_weight=own_weight, send_block=send_block, send_target=send_target, send_count=send_count, send_weight=send_weight, left_block=left_block, left_target=left_target, left_count=left_count, left_weight=left_weight)


def reference(fields, own_src, own_weight, send_block, send_target, send_count, send_weight, left_block, left_target, left_count, left_weight):
    levels = fields.shape[0]
    peers = send_count.shape[1]
    blocks = fields.shape[1] // peers
    comp = fields.shape[2]
    cells = fields.shape[3]
    rounded = fields.astype(jnp.bfloat16).reshape(levels, peers, blocks, comp, cells)
    highest = lax.Precision.HIGHEST

    own_index = own_src.reshape(levels, peers, blocks, 1, 1).astype(jnp.int32)
    own_donor = jnp.take_along_axis(rounded, own_index, axis=2).astype(jnp.float32)
    own_frac = own_weight.reshape(levels, peers, blocks, cells, cells).astype(jnp.float32)
    own = jnp.einsum("lqbmk,lqbki->lqbmi", own_donor, own_frac, precision=highest)

    source_dev = lax.broadcasted_iota(jnp.int32, (peers, 1, 1), 0)
    recv_dev = lax.broadcasted_iota(jnp.int32, (1, peers, 1), 1)
    slot_cap = send_block.shape[3]

    def level_intra(packed):
        flds, blk, tgt, cnt, wts = packed
        donors = flds[source_dev, blk]
        valid = lax.broadcasted_iota(jnp.int32, (1, 1, slot_cap), 2) < cnt[:, :, None]
        donors = jnp.where(valid[..., None, None], donors, jnp.zeros_like(donors))
        contrib = jnp.einsum("spcmk,spcki->spcmi", donors.astype(jnp.float32), wts.astype(jnp.float32), precision=highest)
        receive = (recv_dev * blocks + tgt).reshape(-1).astype(jnp.int32)
        total = jnp.zeros((peers * blocks, comp, cells), jnp.float32)
        return total.at[receive].add(contrib.reshape(-1, comp, cells)).reshape(peers, blocks, comp, cells)

    intra = lax.map(level_intra, (rounded, send_block, send_target, send_count, send_weight))

    left_cap = left_block.shape[3]
    dev_index = lax.broadcasted_iota(jnp.int32, (peers, 1, 1), 0)

    def level_left(packed):
        flds, blk, cnt, wts = packed
        donors = flds[dev_index, blk]
        valid = lax.broadcasted_iota(jnp.int32, (1, 1, left_cap), 2) < cnt[:, :, None]
        donors = jnp.where(valid[..., None, None], donors, jnp.zeros_like(donors))
        return jnp.einsum("qlcmk,qlcki->qlcmi", donors.astype(jnp.float32), wts.astype(jnp.float32), precision=highest)

    left_terms = lax.map(level_left, (rounded, left_block, left_count, left_weight))
    dst_level = lax.broadcasted_iota(jnp.int32, (1, 1, levels, 1), 2)
    dev_here = lax.broadcasted_iota(jnp.int32, (1, peers, 1, 1), 1)
    recv_left = ((dst_level * peers + dev_here) * blocks + left_target).reshape(-1).astype(jnp.int32)
    leftover = jnp.zeros((levels * peers * blocks, comp, cells), jnp.float32)
    leftover = leftover.at[recv_left].add(left_terms.reshape(-1, comp, cells))
    leftover = leftover.reshape(levels, peers, blocks, comp, cells)

    remapped = (own + intra + leftover).reshape(levels, peers * blocks, comp, cells)
    totals = jnp.sum(remapped, axis=(0, 1, 3)) / (CELLS * BLK_DEV)
    return remapped, totals
```

```python
import functools

import jax
import jax.numpy as jnp
from jax import lax
from jax.experimental import pallas as pl
from jax.experimental.pallas import tpu as pltpu
from jax.sharding import PartitionSpec as P

MESH = pl.DeviceIdType.MESH
F32 = jnp.float32
BF16 = jnp.bfloat16


def kernel(
    nd,
    nl,
    own_src,
    send_block,
    send_target,
    send_count,
    left_block,
    left_target,
    left_count,
    fields_hbm,
    own_hbm,
    send_hbm,
    left_hbm,
    out_ref,
    tot_ref,
    fields,
    own_w,
    send_w,
    left_w,
    load_sem,
    sbuf,
    rbuf,
    s_sem,
    r_sem,
    lsbuf,
    lrbuf,
    ls_sem,
    lr_sem,
    tbuf,
    trecv,
    ts_sem,
    tr_sem,
    ubuf,
    urecv,
    us_sem,
    ur_sem,
):
    dev = lax.axis_index("dev")
    lvl = lax.axis_index("level")
    blocks, cells = own_w.shape[:2]
    comp = fields.shape[0] // blocks
    cap = send_w.shape[1]
    lcap = left_w.shape[1]
    rows = sbuf.shape[1] // cap

    loads = [
        pltpu.make_async_copy(src, dst, load_sem.at[i])
        for i, (src, dst) in enumerate(
            ((fields_hbm, fields), (left_hbm, left_w), (send_hbm, send_w), (own_hbm, own_w))
        )
    ]
    for load in loads:
        load.start()

    def dev_peer(r):
        return {"dev": lax.rem(dev + r, nd)}

    def lvl_peer(r):
        return {"level": lax.rem(lvl + r, nl)}

    barrier = pltpu.get_barrier_semaphore()
    for r in range(1, nd):
        pl.semaphore_signal(barrier, inc=1, device_id=dev_peer(r), device_id_type=MESH)
    for r in range(1, nl):
        pl.semaphore_signal(barrier, inc=1, device_id=lvl_peer(r), device_id_type=MESH)

    part = jnp.zeros((comp, cells), F32)

    def donor(index):
        return fields[pl.ds(index, comp, stride=blocks), :]

    def product(block, weight):
        return jnp.dot(block.astype(BF16), weight, preferred_element_type=F32)

    def message(buf, r, c, slot_block, slot_target, slot_count, weights, peer):
        block = donor(slot_block[c, peer])
        block = jnp.where(c < slot_count[0, peer], block, jnp.zeros_like(block))
        term = product(block, weights[peer, c])
        target = jnp.full((rows - comp, cells), slot_target[c, peer].astype(F32), F32)
        buf[r, c * rows : (c + 1) * rows, :] = jnp.concatenate([term, target], axis=0).astype(BF16)
        return term

    loads[0].wait()
    loads[1].wait()
    for r in range(1, nl):
        peer = lax.rem(lvl + r, nl)
        for c in range(lcap):
            part += message(lsbuf, r, c, left_block, left_target, left_count, left_w, peer)
    loads[2].wait()
    for r in range(1, nd):
        peer = lax.rem(dev + r, nd)
        for c in range(cap):
            part += message(sbuf, r, c, send_block, send_target, send_count, send_w, peer)

    pl.semaphore_wait(barrier, nd - 1 + nl - 1)

    sends = []

    def send(src, dst, s, d, who):
        copy = pltpu.make_async_remote_copy(
            src_ref=src, dst_ref=dst, send_sem=s, recv_sem=d, device_id=who, device_id_type=MESH
        )
        copy.start()
        sends.append(copy)
        return copy

    lefts = [
        send(lsbuf.at[r], lrbuf.at[r], ls_sem.at[r], lr_sem.at[r], lvl_peer(r))
        for r in range(1, nl)
    ]
    intras = [
        send(sbuf.at[r], rbuf.at[r], s_sem.at[r], r_sem.at[r], dev_peer(r)) for r in range(1, nd)
    ]

    loads[3].wait()
    acc = []
    for b in range(blocks):
        term = product(donor(own_src[0, b]), own_w[b])
        part += term
        acc.append(term)

    sums = jnp.sum(part, axis=1, keepdims=True)
    same = lax.broadcasted_iota(jnp.int32, (comp, cells), 0) == lax.broadcasted_iota(
        jnp.int32, (comp, cells), 1
    )
    row = jnp.sum(jnp.where(same, sums, 0.0), axis=0, keepdims=True)
    tbuf[...] = row
    tots = [
        send(tbuf, trecv.at[r], ts_sem.at[r], tr_sem.at[r], dev_peer(r)) for r in range(1, nd)
    ]
    for r, copy in enumerate(tots, 1):
        copy.wait_recv()
        row += trecv[r]
    ubuf[...] = row
    tops = [
        send(ubuf, urecv.at[r], us_sem.at[r], ur_sem.at[r], lvl_peer(r)) for r in range(1, nl)
    ]

    def place(buf, r, slots):
        for c in range(slots):
            got = buf[r, c * rows : (c + 1) * rows, :].astype(F32)
            term = got[:comp]
            target = jnp.broadcast_to(got[comp : comp + 1], (comp, cells))
            for b in range(blocks):
                acc[b] = acc[b] + jnp.where(target == float(b), term, 0.0)

    for r, copy in enumerate(intras, 1):
        copy.wait_recv()
        place(rbuf, r, cap)
    for r, copy in enumerate(lefts, 1):
        copy.wait_recv()
        place(lrbuf, r, lcap)
    for b in range(blocks):
        out_ref[pl.ds(b, comp, stride=blocks), :] = acc[b]
    for r, copy in enumerate(tops, 1):
        copy.wait_recv()
        row += urecv[r]
    tot_ref[...] = (row / (cells * blocks))[0, :comp]
    for copy in sends:
        copy.wait_send()


def solution(mesh):
    nd = mesh.shape["dev"]
    nl = mesh.shape["level"]

    def body(
        fields,
        own_src,
        own_weight,
        send_block,
        send_target,
        send_count,
        send_weight,
        left_block,
        left_target,
        left_count,
        left_weight,
    ):
        blocks, comp, cells = fields.shape[1:]
        cap = send_weight.shape[3]
        lcap = left_weight.shape[3]
        rows = -(-(comp + 1) // 16) * 16
        smem = pl.BlockSpec(memory_space=pltpu.SMEM)
        hbm = pl.BlockSpec(memory_space=pl.ANY)
        vmem = pl.BlockSpec(memory_space=pltpu.VMEM)
        dma = pltpu.SemaphoreType.DMA
        remapped, totals = pl.pallas_call(
            functools.partial(kernel, nd, nl),
            out_shape=(
                jax.ShapeDtypeStruct((comp * blocks, cells), F32),
                jax.ShapeDtypeStruct((comp,), F32),
            ),
            in_specs=[smem] * 7 + [hbm] * 4,
            out_specs=(vmem, vmem),
            scratch_shapes=[
                pltpu.VMEM((comp * blocks, cells), F32),
                pltpu.VMEM((blocks, cells, cells), BF16),
                pltpu.VMEM((nd, cap, cells, cells), BF16),
                pltpu.VMEM((nl, lcap, cells, cells), BF16),
                dma((4,)),
                pltpu.VMEM((nd, cap * rows, cells), BF16),
                pltpu.VMEM((nd, cap * rows, cells), BF16),
                dma((nd,)),
                dma((nd,)),
                pltpu.VMEM((nl, lcap * rows, cells), BF16),
                pltpu.VMEM((nl, lcap * rows, cells), BF16),
                dma((nl,)),
                dma((nl,)),
                pltpu.VMEM((1, cells), F32),
                pltpu.VMEM((nd, 1, cells), F32),
                dma((nd,)),
                dma((nd,)),
                pltpu.VMEM((1, cells), F32),
                pltpu.VMEM((nl, 1, cells), F32),
                dma((nl,)),
                dma((nl,)),
            ],
            compiler_params=pltpu.CompilerParams(collective_id=0, has_side_effects=True),
        )(
            own_src,
            send_block[0, 0].T,
            send_target[0, 0].T,
            send_count[0],
            left_block[0, 0].T,
            left_target[0, 0].T,
            left_count[0],
            fields[0].transpose(1, 0, 2).reshape(comp * blocks, cells),
            own_weight[0],
            send_weight[0, 0],
            left_weight[0, 0],
        )
        remapped = remapped.reshape(comp, blocks, cells).transpose(1, 0, 2)
        return remapped[None], totals

    in_specs = (
        P("level", "dev", None, None),
        P("level", "dev"),
        P("level", "dev", None, None),
        P("level", "dev", None, None),
        P("level", "dev", None, None),
        P("level", "dev", None),
        P("level", "dev", None, None, None, None),
        P("level", "dev", None, None),
        P("level", "dev", None, None),
        P("level", "dev", None),
        P("level", "dev", None, None, None, None),
    )
    out_specs = (P("level", "dev", None, None), P())
    return jax.shard_map(body, mesh=mesh, in_specs=in_specs, out_specs=out_specs, check_vma=False)
```

```python
import functools

import jax
import jax.numpy as jnp
from jax import lax
from jax.experimental import pallas as pl
from jax.experimental.pallas import tpu as pltpu
from jax.sharding import PartitionSpec as P

MESH = pl.DeviceIdType.MESH
F32 = jnp.float32
BF16 = jnp.bfloat16


def kernel(
    nd,
    nl,
    own_src_hbm,
    send_block_hbm,
    send_target_hbm,
    send_count_hbm,
    left_block_hbm,
    left_target_hbm,
    left_count_hbm,
    fields_hbm,
    own_hbm,
    send_hbm,
    left_hbm,
    out_ref,
    tot_ref,
    own_src,
    send_block,
    send_target,
    send_count,
    left_block,
    left_target,
    left_count,
    fields,
    own_w,
    send_w,
    left_w,
    load_sem,
    sbuf,
    rbuf,
    s_sem,
    r_sem,
    lsbuf,
    lrbuf,
    ls_sem,
    lr_sem,
    tbuf,
    trecv,
    ts_sem,
    tr_sem,
    ubuf,
    urecv,
    us_sem,
    ur_sem,
):
    dev = lax.axis_index("dev")
    lvl = lax.axis_index("level")
    blocks, cells = own_w.shape[:2]
    comp = fields.shape[0] // blocks
    cap = send_w.shape[1]
    lcap = left_w.shape[1]
    rows = sbuf.shape[1] // cap

    def dev_peer(r):
        return {"dev": lax.rem(dev + r, nd)}

    def lvl_peer(r):
        return {"level": lax.rem(lvl + r, nl)}

    barrier = pltpu.get_barrier_semaphore()
    for r in range(1, nd):
        pl.semaphore_signal(barrier, inc=1, device_id=dev_peer(r), device_id_type=MESH)
    for r in range(1, nl):
        pl.semaphore_signal(barrier, inc=1, device_id=lvl_peer(r), device_id_type=MESH)

    pairs = (
        (left_block_hbm, left_block),
        (left_target_hbm, left_target),
        (left_count_hbm, left_count),
        (fields_hbm, fields),
        (left_hbm, left_w),
        (send_block_hbm, send_block),
        (send_target_hbm, send_target),
        (send_count_hbm, send_count),
        (send_hbm, send_w),
        (own_src_hbm, own_src),
        (own_hbm, own_w),
    )
    loads = [
        pltpu.make_async_copy(src, dst, load_sem.at[i]) for i, (src, dst) in enumerate(pairs)
    ]
    for load in loads:
        load.start()

    part = jnp.zeros((comp, cells), F32)

    def donor(index):
        return fields[pl.ds(index, comp, stride=blocks), :]

    def product(block, weight):
        return jnp.dot(block.astype(BF16), weight, preferred_element_type=F32)

    def message(buf, r, c, slot_block, slot_target, slot_count, weights, peer):
        block = donor(slot_block[c, peer])
        block = jnp.where(c < slot_count[0, peer], block, jnp.zeros_like(block))
        term = product(block, weights[peer, c])
        target = jnp.full((rows - comp, cells), slot_target[c, peer].astype(F32), F32)
        buf[r, c * rows : (c + 1) * rows, :] = jnp.concatenate([term, target], axis=0).astype(BF16)
        return term

    for load in loads[:5]:
        load.wait()
    for r in range(1, nl):
        peer = lax.rem(lvl + r, nl)
        for c in range(lcap):
            part += message(lsbuf, r, c, left_block, left_target, left_count, left_w, peer)
    for load in loads[5:9]:
        load.wait()
    for r in range(1, nd):
        peer = lax.rem(dev + r, nd)
        for c in range(cap):
            part += message(sbuf, r, c, send_block, send_target, send_count, send_w, peer)

    pl.semaphore_wait(barrier, nd - 1 + nl - 1)

    sends = []

    def send(src, dst, s, d, who):
        copy = pltpu.make_async_remote_copy(
            src_ref=src, dst_ref=dst, send_sem=s, recv_sem=d, device_id=who, device_id_type=MESH
        )
        copy.start()
        sends.append(copy)
        return copy

    lefts = [
        send(lsbuf.at[r], lrbuf.at[r], ls_sem.at[r], lr_sem.at[r], lvl_peer(r))
        for r in range(1, nl)
    ]
    intras = [
        send(sbuf.at[r], rbuf.at[r], s_sem.at[r], r_sem.at[r], dev_peer(r)) for r in range(1, nd)
    ]

    for load in loads[9:]:
        load.wait()
    acc = []
    for b in range(blocks):
        term = product(donor(own_src[0, b]), own_w[b])
        part += term
        acc.append(term)

    sums = jnp.sum(part, axis=1, keepdims=True)
    same = lax.broadcasted_iota(jnp.int32, (comp, cells), 0) == lax.broadcasted_iota(
        jnp.int32, (comp, cells), 1
    )
    row = jnp.sum(jnp.where(same, sums, 0.0), axis=0, keepdims=True)
    tbuf[...] = row
    tots = [
        send(tbuf, trecv.at[r], ts_sem.at[r], tr_sem.at[r], dev_peer(r)) for r in range(1, nd)
    ]
    for r, copy in enumerate(tots, 1):
        copy.wait_recv()
        row += trecv[r]
    ubuf[...] = row
    tops = [
        send(ubuf, urecv.at[r], us_sem.at[r], ur_sem.at[r], lvl_peer(r)) for r in range(1, nl)
    ]

    def place(buf, r, slots):
        for c in range(slots):
            got = buf[r, c * rows : (c + 1) * rows, :].astype(F32)
            term = got[:comp]
            target = jnp.broadcast_to(got[comp : comp + 1], (comp, cells))
            for b in range(blocks):
                acc[b] = acc[b] + jnp.where(target == float(b), term, 0.0)

    for r, copy in enumerate(intras, 1):
        copy.wait_recv()
        place(rbuf, r, cap)
    for r, copy in enumerate(lefts, 1):
        copy.wait_recv()
        place(lrbuf, r, lcap)
    for b in range(blocks):
        out_ref[pl.ds(b, comp, stride=blocks), :] = acc[b]
    for r, copy in enumerate(tops, 1):
        copy.wait_recv()
        row += urecv[r]
    tot_ref[...] = (row / (cells * blocks))[0, :comp]
    for copy in sends:
        copy.wait_send()


def solution(mesh):
    nd = mesh.shape["dev"]
    nl = mesh.shape["level"]

    def body(
        fields,
        own_src,
        own_weight,
        send_block,
        send_target,
        send_count,
        send_weight,
        left_block,
        left_target,
        left_count,
        left_weight,
    ):
        blocks, comp, cells = fields.shape[1:]
        cap = send_weight.shape[3]
        lcap = left_weight.shape[3]
        rows = -(-(comp + 1) // 16) * 16
        smem = functools.partial(pltpu.SMEM, dtype=jnp.int32)
        hbm = pl.BlockSpec(memory_space=pl.ANY)
        vmem = pl.BlockSpec(memory_space=pltpu.VMEM)
        dma = pltpu.SemaphoreType.DMA
        remapped, totals = pl.pallas_call(
            functools.partial(kernel, nd, nl),
            out_shape=(
                pltpu.VMEM((comp * blocks, cells), F32),
                pltpu.VMEM((comp,), F32),
            ),
            in_specs=[hbm] * 11,
            out_specs=(vmem, vmem),
            scratch_shapes=[
                smem((1, blocks)),
                smem((cap, nd)),
                smem((cap, nd)),
                smem((1, nd)),
                smem((lcap, nl)),
                smem((lcap, nl)),
                smem((1, nl)),
                pltpu.VMEM((comp * blocks, cells), F32),
                pltpu.VMEM((blocks, cells, cells), BF16),
                pltpu.VMEM((nd, cap, cells, cells), BF16),
                pltpu.VMEM((nl, lcap, cells, cells), BF16),
                dma((11,)),
                pltpu.VMEM((nd, cap * rows, cells), BF16),
                pltpu.VMEM((nd, cap * rows, cells), BF16),
                dma((nd,)),
                dma((nd,)),
                pltpu.VMEM((nl, lcap * rows, cells), BF16),
                pltpu.VMEM((nl, lcap * rows, cells), BF16),
                dma((nl,)),
                dma((nl,)),
                pltpu.VMEM((1, cells), F32),
                pltpu.VMEM((nd, 1, cells), F32),
                dma((nd,)),
                dma((nd,)),
                pltpu.VMEM((1, cells), F32),
                pltpu.VMEM((nl, 1, cells), F32),
                dma((nl,)),
                dma((nl,)),
            ],
            compiler_params=pltpu.CompilerParams(collective_id=0, has_side_effects=True),
        )(
            own_src,
            send_block[0, 0].T,
            send_target[0, 0].T,
            send_count[0],
            left_block[0, 0].T,
            left_target[0, 0].T,
            left_count[0],
            fields[0].transpose(1, 0, 2).reshape(comp * blocks, cells),
            own_weight[0],
            send_weight[0, 0],
            left_weight[0, 0],
        )
        remapped = remapped.reshape(comp, blocks, cells).transpose(1, 0, 2)
        return remapped[None], totals

    in_specs = (
        P("level", "dev", None, None),
        P("level", "dev"),
        P("level", "dev", None, None),
        P("level", "dev", None, None),
        P("level", "dev", None, None),
        P("level", "dev", None),
        P("level", "dev", None, None, None, None),
        P("level", "dev", None, None),
        P("level", "dev", None, None),
        P("level", "dev", None),
        P("level", "dev", None, None, None, None),
    )
    out_specs = (P("level", "dev", None, None), P())
    return jax.shard_map(body, mesh=mesh, in_specs=in_specs, out_specs=out_specs, check_vma=False)
```

```python
import functools

import jax
import jax.numpy as jnp
from jax import lax
from jax.experimental import pallas as pl
from jax.experimental.pallas import tpu as pltpu
from jax.sharding import PartitionSpec as P

MESH = pl.DeviceIdType.MESH
F32 = jnp.float32
BF16 = jnp.bfloat16


def kernel(
    nd,
    nl,
    direct,
    own_src_hbm,
    send_block_hbm,
    send_target_hbm,
    send_count_hbm,
    left_block_hbm,
    left_target_hbm,
    left_count_hbm,
    fields_hbm,
    own_hbm,
    send_hbm,
    left_hbm,
    out_ref,
    tot_ref,
    own_src,
    send_block,
    send_target,
    send_count,
    left_block,
    left_target,
    left_count,
    fields,
    own_w,
    send_w,
    left_w,
    load_sem,
    sbuf,
    rbuf,
    s_sem,
    r_sem,
    lsbuf,
    lrbuf,
    ls_sem,
    lr_sem,
    tbuf,
    trecv,
    ts_sem,
    tr_sem,
    ubuf,
    urecv,
    us_sem,
    ur_sem,
):
    dev = lax.axis_index("dev")
    lvl = lax.axis_index("level")
    blocks, cells = own_w.shape[:2]
    comp = fields.shape[0] // blocks
    cap = send_w.shape[1]
    lcap = left_w.shape[1]
    rows = sbuf.shape[1] // cap

    barrier = pltpu.get_barrier_semaphore()
    def peer_of(l, r):
        return {"level": lax.rem(lvl + l, nl), "dev": lax.rem(dev + r, nd)}

    offsets = [
        (l, r)
        for l in range(nl)
        for r in range(nd)
        if (l or r) and (direct or not (l and r))
    ]
    for l, r in offsets:
        pl.semaphore_signal(barrier, inc=1, device_id=peer_of(l, r), device_id_type=MESH)

    left_peers = [lax.rem(lvl + r, nl) for r in range(1, nl)]
    send_peers = [lax.rem(dev + r, nd) for r in range(1, nd)]
    pairs = (
        (left_block_hbm, left_block),
        (left_target_hbm, left_target),
        (left_count_hbm, left_count),
        (fields_hbm, fields),
        *[(left_hbm.at[p], left_w.at[p]) for p in left_peers],
        (send_block_hbm, send_block),
        (send_target_hbm, send_target),
        (send_count_hbm, send_count),
        *[(send_hbm.at[p], send_w.at[p]) for p in send_peers],
        (own_src_hbm, own_src),
        (own_hbm, own_w),
    )
    loads = [
        pltpu.make_async_copy(src, dst, load_sem.at[i]) for i, (src, dst) in enumerate(pairs)
    ]
    for load in loads:
        load.start()

    part = jnp.zeros((comp, cells), F32)

    def donor(index):
        return fields[pl.ds(index, comp, stride=blocks), :]

    def product(block, weight):
        return jnp.dot(block.astype(BF16), weight, preferred_element_type=F32)

    def message(buf, r, c, slot_block, slot_target, slot_count, weights, peer):
        block = donor(slot_block[c, peer])
        block = jnp.where(c < slot_count[0, peer], block, jnp.zeros_like(block))
        term = product(block, weights[peer, c])
        target = jnp.full((rows - comp, cells), slot_target[c, peer].astype(F32), F32)
        buf[r, c * rows : (c + 1) * rows, :] = jnp.concatenate([term, target], axis=0).astype(BF16)
        return term

    first = 4 + len(left_peers)
    second = first + 3 + len(send_peers)
    for load in loads[:first]:
        load.wait()
    for r in range(1, nl):
        peer = lax.rem(lvl + r, nl)
        for c in range(lcap):
            part += message(lsbuf, r, c, left_block, left_target, left_count, left_w, peer)
    for load in loads[first:second]:
        load.wait()
    for r in range(1, nd):
        peer = lax.rem(dev + r, nd)
        for c in range(cap):
            part += message(sbuf, r, c, send_block, send_target, send_count, send_w, peer)

    pl.semaphore_wait(barrier, len(offsets))

    sends = []

    def send(src, dst, s, d, who):
        copy = pltpu.make_async_remote_copy(
            src_ref=src, dst_ref=dst, send_sem=s, recv_sem=d, device_id=who, device_id_type=MESH
        )
        copy.start()
        sends.append(copy)
        return copy

    lefts = [
        send(lsbuf.at[r], lrbuf.at[r], ls_sem.at[r], lr_sem.at[r], peer_of(r, 0))
        for r in range(1, nl)
    ]
    intras = [
        send(sbuf.at[r], rbuf.at[r], s_sem.at[r], r_sem.at[r], peer_of(0, r)) for r in range(1, nd)
    ]

    for load in loads[second:]:
        load.wait()
    acc = []
    for b in range(blocks):
        term = product(donor(own_src[0, b]), own_w[b])
        part += term
        acc.append(term)

    sums = jnp.sum(part, axis=1, keepdims=True)
    same = lax.broadcasted_iota(jnp.int32, (comp, cells), 0) == lax.broadcasted_iota(
        jnp.int32, (comp, cells), 1
    )
    row = jnp.sum(jnp.where(same, sums, 0.0), axis=0, keepdims=True)
    tbuf[...] = row
    if direct:
        tops = [
            send(tbuf, urecv.at[i], us_sem.at[i], ur_sem.at[i], peer_of(l, r))
            for i, (l, r) in enumerate(offsets)
        ]
    else:
        tots = [
            send(tbuf, trecv.at[r], ts_sem.at[r], tr_sem.at[r], peer_of(0, r))
            for r in range(1, nd)
        ]
        for r, copy in enumerate(tots, 1):
            copy.wait_recv()
            row += trecv[r]
        ubuf[...] = row
        tops = [
            send(ubuf, urecv.at[i], us_sem.at[i], ur_sem.at[i], peer_of(i + 1, 0))
            for i in range(nl - 1)
        ]

    def place(buf, r, slots):
        for c in range(slots):
            got = buf[r, c * rows : (c + 1) * rows, :].astype(F32)
            term = got[:comp]
            target = jnp.broadcast_to(got[comp : comp + 1], (comp, cells))
            for b in range(blocks):
                acc[b] = acc[b] + jnp.where(target == float(b), term, 0.0)

    for r, copy in enumerate(intras, 1):
        copy.wait_recv()
        place(rbuf, r, cap)
    for r, copy in enumerate(lefts, 1):
        copy.wait_recv()
        place(lrbuf, r, lcap)
    for b in range(blocks):
        out_ref[pl.ds(b, comp, stride=blocks), :] = acc[b]
    for copy in tops:
        copy.wait_recv()
    terms = [row] + [urecv[i] for i in range(len(tops))]
    while len(terms) > 1:
        half = len(terms) // 2
        terms = [a + b for a, b in zip(terms[:half], terms[half:])] + terms[2 * half :]
    row = terms[0]
    tot_ref[...] = (row / (cells * blocks))[0, :comp]
    for copy in sends:
        copy.wait_send()


def solution(mesh):
    nd = mesh.shape["dev"]
    nl = mesh.shape["level"]
    direct = nd * nl <= 64
    last = (nd if direct else 1) * nl

    def body(
        fields,
        own_src,
        own_weight,
        send_block,
        send_target,
        send_count,
        send_weight,
        left_block,
        left_target,
        left_count,
        left_weight,
    ):
        blocks, comp, cells = fields.shape[1:]
        cap = send_weight.shape[3]
        lcap = left_weight.shape[3]
        rows = -(-(comp + 1) // 16) * 16
        smem = functools.partial(pltpu.SMEM, dtype=jnp.int32)
        hbm = pl.BlockSpec(memory_space=pl.ANY)
        vmem = pl.BlockSpec(memory_space=pltpu.VMEM)
        dma = pltpu.SemaphoreType.DMA
        remapped, totals = pl.pallas_call(
            functools.partial(kernel, nd, nl, direct),
            out_shape=(
                pltpu.VMEM((comp * blocks, cells), F32),
                pltpu.VMEM((comp,), F32),
            ),
            in_specs=[hbm] * 11,
            out_specs=(vmem, vmem),
            scratch_shapes=[
                smem((1, blocks)),
                smem((cap, nd)),
                smem((cap, nd)),
                smem((1, nd)),
                smem((lcap, nl)),
                smem((lcap, nl)),
                smem((1, nl)),
                pltpu.VMEM((comp * blocks, cells), F32),
                pltpu.VMEM((blocks, cells, cells), BF16),
                pltpu.VMEM((nd, cap, cells, cells), BF16),
                pltpu.VMEM((nl, lcap, cells, cells), BF16),
                dma((9 + nd + nl,)),
                pltpu.VMEM((nd, cap * rows, cells), BF16),
                pltpu.VMEM((nd, cap * rows, cells), BF16),
                dma((nd,)),
                dma((nd,)),
                pltpu.VMEM((nl, lcap * rows, cells), BF16),
                pltpu.VMEM((nl, lcap * rows, cells), BF16),
                dma((nl,)),
                dma((nl,)),
                pltpu.VMEM((1, cells), F32),
                pltpu.VMEM((nd, 1, cells), F32),
                dma((nd,)),
                dma((nd,)),
                pltpu.VMEM((1, cells), F32),
                pltpu.VMEM((last, 1, cells), F32),
                dma((last,)),
                dma((last,)),
            ],
            compiler_params=pltpu.CompilerParams(collective_id=0, has_side_effects=True),
        )(
            own_src,
            send_block[0, 0].T,
            send_target[0, 0].T,
            send_count[0],
            left_block[0, 0].T,
            left_target[0, 0].T,
            left_count[0],
            fields[0].transpose(1, 0, 2).reshape(comp * blocks, cells),
            own_weight[0],
            send_weight[0, 0],
            left_weight[0, 0],
        )
        remapped = remapped.reshape(comp, blocks, cells).transpose(1, 0, 2)
        return remapped[None], totals

    in_specs = (
        P("level", "dev", None, None),
        P("level", "dev"),
        P("level", "dev", None, None),
        P("level", "dev", None, None),
        P("level", "dev", None, None),
        P("level", "dev", None),
        P("level", "dev", None, None, None, None),
        P("level", "dev", None, None),
        P("level", "dev", None, None),
        P("level", "dev", None),
        P("level", "dev", None, None, None, None),
    )
    out_specs = (P("level", "dev", None, None), P())
    return jax.shard_map(body, mesh=mesh, in_specs=in_specs, out_specs=out_specs, check_vma=False)
```

```python
import functools

import jax
import jax.numpy as jnp
from jax import lax
from jax.experimental import pallas as pl
from jax.experimental.pallas import tpu as pltpu
from jax.sharding import PartitionSpec as P

MESH = pl.DeviceIdType.MESH
F32 = jnp.float32
BF16 = jnp.bfloat16


def kernel(
    nd,
    nl,
    direct,
    own_src_hbm,
    send_block_hbm,
    send_target_hbm,
    send_count_hbm,
    left_block_hbm,
    left_target_hbm,
    left_count_hbm,
    fields_hbm,
    own_hbm,
    send_hbm,
    left_hbm,
    out_ref,
    tot_ref,
    own_src,
    send_block,
    send_target,
    send_count,
    left_block,
    left_target,
    left_count,
    fields,
    own_w,
    send_w,
    left_w,
    load_sem,
    sbuf,
    rbuf,
    s_sem,
    r_sem,
    lsbuf,
    lrbuf,
    ls_sem,
    lr_sem,
    tbuf,
    trecv,
    ts_sem,
    tr_sem,
    ubuf,
    urecv,
    us_sem,
    ur_sem,
):
    dev = lax.axis_index("dev")
    lvl = lax.axis_index("level")
    blocks, cells = own_w.shape[:2]
    comp = fields.shape[0] // blocks
    cap = send_w.shape[1]
    lcap = left_w.shape[1]
    rows = sbuf.shape[1] // cap

    barrier = pltpu.get_barrier_semaphore()
    left_peers = [lax.rem(lvl + r, nl) for r in range(1, nl)]
    send_peers = [lax.rem(dev + r, nd) for r in range(1, nd)]
    pairs = (
        (left_block_hbm, left_block),
        (left_target_hbm, left_target),
        (left_count_hbm, left_count),
        (fields_hbm, fields),
        *[(left_hbm.at[p], left_w.at[p]) for p in left_peers],
        (send_block_hbm, send_block),
        (send_target_hbm, send_target),
        (send_count_hbm, send_count),
        *[(send_hbm.at[p], send_w.at[p]) for p in send_peers],
        (own_src_hbm, own_src),
        (own_hbm, own_w),
    )
    loads = [
        pltpu.make_async_copy(src, dst, load_sem.at[i]) for i, (src, dst) in enumerate(pairs)
    ]
    for load in loads:
        load.start()

    def peer_of(l, r):
        return {"level": lax.rem(lvl + l, nl), "dev": lax.rem(dev + r, nd)}

    offsets = [
        (l, r)
        for l in reversed(range(nl))
        for r in reversed(range(nd))
        if (l or r) and (direct or not (l and r))
    ]
    for l, r in offsets:
        pl.semaphore_signal(barrier, inc=1, device_id=peer_of(l, r), device_id_type=MESH)

    part = jnp.zeros((comp, cells), F32)

    def donor(index):
        return fields[pl.ds(index, comp, stride=blocks), :]

    def product(block, weight):
        return jnp.dot(block.astype(BF16), weight, preferred_element_type=F32)

    def message(buf, r, c, slot_block, slot_target, slot_count, weights, peer):
        block = donor(slot_block[c, peer])
        block = jnp.where(c < slot_count[0, peer], block, jnp.zeros_like(block))
        term = product(block, weights[peer, c])
        target = jnp.full((rows - comp, cells), slot_target[c, peer].astype(F32), F32)
        buf[r, c * rows : (c + 1) * rows, :] = jnp.concatenate([term, target], axis=0).astype(BF16)
        return term

    first = 4 + len(left_peers)
    second = first + 3 + len(send_peers)
    for load in loads[:first]:
        load.wait()
    for r in range(1, nl):
        peer = lax.rem(lvl + r, nl)
        for c in range(lcap):
            part += message(lsbuf, r, c, left_block, left_target, left_count, left_w, peer)
    for load in loads[first:second]:
        load.wait()
    for r in range(1, nd):
        peer = lax.rem(dev + r, nd)
        for c in range(cap):
            part += message(sbuf, r, c, send_block, send_target, send_count, send_w, peer)

    for load in loads[second:]:
        load.wait()
    acc = []
    for b in range(blocks):
        term = product(donor(own_src[0, b]), own_w[b])
        part += term
        acc.append(term)

    sums = jnp.sum(part, axis=1, keepdims=True)
    same = lax.broadcasted_iota(jnp.int32, (comp, cells), 0) == lax.broadcasted_iota(
        jnp.int32, (comp, cells), 1
    )
    row = jnp.sum(jnp.where(same, sums, 0.0), axis=0, keepdims=True)
    tbuf[...] = row

    pl.semaphore_wait(barrier, len(offsets))

    sends = []

    def send(src, dst, s, d, who):
        copy = pltpu.make_async_remote_copy(
            src_ref=src, dst_ref=dst, send_sem=s, recv_sem=d, device_id=who, device_id_type=MESH
        )
        copy.start()
        sends.append(copy)
        return copy

    if direct:
        tops = [
            send(tbuf, urecv.at[i], us_sem.at[i], ur_sem.at[i], peer_of(l, r))
            for i, (l, r) in enumerate(offsets)
        ]
    else:
        tots = [
            send(tbuf, trecv.at[r], ts_sem.at[r], tr_sem.at[r], peer_of(0, r))
            for r in range(1, nd)
        ]
    lefts = [
        send(lsbuf.at[r], lrbuf.at[r], ls_sem.at[r], lr_sem.at[r], peer_of(r, 0))
        for r in range(1, nl)
    ]
    intras = [
        send(sbuf.at[r], rbuf.at[r], s_sem.at[r], r_sem.at[r], peer_of(0, r)) for r in range(1, nd)
    ]
    if not direct:
        for r, copy in enumerate(tots, 1):
            copy.wait_recv()
            row += trecv[r]
        ubuf[...] = row
        tops = [
            send(ubuf, urecv.at[i], us_sem.at[i], ur_sem.at[i], peer_of(i + 1, 0))
            for i in range(nl - 1)
        ]

    def place(buf, r, slots):
        for c in range(slots):
            got = buf[r, c * rows : (c + 1) * rows, :].astype(F32)
            term = got[:comp]
            target = jnp.broadcast_to(got[comp : comp + 1], (comp, cells))
            for b in range(blocks):
                acc[b] = acc[b] + jnp.where(target == float(b), term, 0.0)

    for r, copy in enumerate(intras, 1):
        copy.wait_recv()
        place(rbuf, r, cap)
    for r, copy in enumerate(lefts, 1):
        copy.wait_recv()
        place(lrbuf, r, lcap)
    for b in range(blocks):
        out_ref[pl.ds(b, comp, stride=blocks), :] = acc[b]
    for copy in sends:
        copy.wait_send()
    for copy in tops:
        copy.wait_recv()
    terms = [row] + [urecv[i] for i in range(len(tops))]
    while len(terms) > 1:
        half = len(terms) // 2
        terms = [a + b for a, b in zip(terms[:half], terms[half:])] + terms[2 * half :]
    row = terms[0]
    tot_ref[...] = (row / (cells * blocks))[0, :comp]


def solution(mesh):
    nd = mesh.shape["dev"]
    nl = mesh.shape["level"]
    direct = nd * nl <= 64
    last = (nd if direct else 1) * nl

    def body(
        fields,
        own_src,
        own_weight,
        send_block,
        send_target,
        send_count,
        send_weight,
        left_block,
        left_target,
        left_count,
        left_weight,
    ):
        blocks, comp, cells = fields.shape[1:]
        cap = send_weight.shape[3]
        lcap = left_weight.shape[3]
        rows = -(-(comp + 1) // 16) * 16
        smem = functools.partial(pltpu.SMEM, dtype=jnp.int32)
        hbm = pl.BlockSpec(memory_space=pl.ANY)
        vmem = pl.BlockSpec(memory_space=pltpu.VMEM)
        dma = pltpu.SemaphoreType.DMA
        remapped, totals = pl.pallas_call(
            functools.partial(kernel, nd, nl, direct),
            out_shape=(
                pltpu.VMEM((comp * blocks, cells), F32),
                pltpu.VMEM((comp,), F32),
            ),
            in_specs=[hbm] * 11,
            out_specs=(vmem, vmem),
            scratch_shapes=[
                smem((1, blocks)),
                smem((cap, nd)),
                smem((cap, nd)),
                smem((1, nd)),
                smem((lcap, nl)),
                smem((lcap, nl)),
                smem((1, nl)),
                pltpu.VMEM((comp * blocks, cells), F32),
                pltpu.VMEM((blocks, cells, cells), BF16),
                pltpu.VMEM((nd, cap, cells, cells), BF16),
                pltpu.VMEM((nl, lcap, cells, cells), BF16),
                dma((9 + nd + nl,)),
                pltpu.VMEM((nd, cap * rows, cells), BF16),
                pltpu.VMEM((nd, cap * rows, cells), BF16),
                dma((nd,)),
                dma((nd,)),
                pltpu.VMEM((nl, lcap * rows, cells), BF16),
                pltpu.VMEM((nl, lcap * rows, cells), BF16),
                dma((nl,)),
                dma((nl,)),
                pltpu.VMEM((1, cells), F32),
                pltpu.VMEM((nd, 1, cells), F32),
                dma((nd,)),
                dma((nd,)),
                pltpu.VMEM((1, cells), F32),
                pltpu.VMEM((last, 1, cells), F32),
                dma((last,)),
                dma((last,)),
            ],
            compiler_params=pltpu.CompilerParams(collective_id=0, has_side_effects=True),
        )(
            own_src,
            send_block[0, 0].T,
            send_target[0, 0].T,
            send_count[0],
            left_block[0, 0].T,
            left_target[0, 0].T,
            left_count[0],
            fields[0].transpose(1, 0, 2).reshape(comp * blocks, cells),
            own_weight[0],
            send_weight[0, 0],
            left_weight[0, 0],
        )
        remapped = remapped.reshape(comp, blocks, cells).transpose(1, 0, 2)
        return remapped[None], totals

    in_specs = (
        P("level", "dev", None, None),
        P("level", "dev"),
        P("level", "dev", None, None),
        P("level", "dev", None, None),
        P("level", "dev", None, None),
        P("level", "dev", None),
        P("level", "dev", None, None, None, None),
        P("level", "dev", None, None),
        P("level", "dev", None, None),
        P("level", "dev", None),
        P("level", "dev", None, None, None, None),
    )
    out_specs = (P("level", "dev", None, None), P())
    return jax.shard_map(body, mesh=mesh, in_specs=in_specs, out_specs=out_specs, check_vma=False)
```

```python
import functools

import jax
import jax.numpy as jnp
from jax import lax
from jax.experimental import pallas as pl
from jax.experimental.pallas import tpu as pltpu
from jax.sharding import PartitionSpec as P

MESH = pl.DeviceIdType.MESH
F32 = jnp.float32
BF16 = jnp.bfloat16


def kernel(
    nd,
    nl,
    direct,
    own_src_hbm,
    send_block_hbm,
    send_target_hbm,
    send_count_hbm,
    left_block_hbm,
    left_target_hbm,
    left_count_hbm,
    fields_hbm,
    own_hbm,
    send_hbm,
    left_hbm,
    out_ref,
    tot_ref,
    own_src,
    send_block,
    send_target,
    send_count,
    left_block,
    left_target,
    left_count,
    fields,
    own_w,
    send_w,
    left_w,
    load_sem,
    sbuf,
    rbuf,
    s_sem,
    r_sem,
    lsbuf,
    lrbuf,
    ls_sem,
    lr_sem,
    tbuf,
    trecv,
    ts_sem,
    tr_sem,
    ubuf,
    urecv,
    us_sem,
    ur_sem,
    entered,
):
    dev = lax.axis_index("dev")
    lvl = lax.axis_index("level")
    blocks, cells = own_w.shape[:2]
    comp = fields.shape[0] // blocks
    cap = send_w.shape[1]
    lcap = left_w.shape[1]
    rows = sbuf.shape[1] // cap

    barrier = pltpu.get_barrier_semaphore()
    left_peers = [lax.rem(lvl + r, nl) for r in range(1, nl)]
    send_peers = [lax.rem(dev + r, nd) for r in range(1, nd)]
    pairs = (
        (left_block_hbm, left_block),
        (left_target_hbm, left_target),
        (left_count_hbm, left_count),
        (fields_hbm, fields),
        *[(left_hbm.at[p], left_w.at[p]) for p in left_peers],
        (send_block_hbm, send_block),
        (send_target_hbm, send_target),
        (send_count_hbm, send_count),
        *[(send_hbm.at[p], send_w.at[p]) for p in send_peers],
        (own_src_hbm, own_src),
        (own_hbm, own_w),
    )
    loads = [
        pltpu.make_async_copy(src, dst, load_sem.at[i]) for i, (src, dst) in enumerate(pairs)
    ]
    for load in loads:
        load.start()

    def peer_of(l, r):
        return {"level": lax.rem(lvl + l, nl), "dev": lax.rem(dev + r, nd)}

    offsets = [
        (l, r)
        for l in reversed(range(nl))
        for r in reversed(range(nd))
        if (l or r) and (direct or not (l and r))
    ]
    near = [(l, r) for l, r in offsets if not (l and r)]
    for l, r in near:
        pl.semaphore_signal(barrier, inc=1, device_id=peer_of(l, r), device_id_type=MESH)

    part = jnp.zeros((comp, cells), F32)

    def donor(index):
        return fields[pl.ds(index, comp, stride=blocks), :]

    def product(block, weight):
        return jnp.dot(block.astype(BF16), weight, preferred_element_type=F32)

    def message(buf, r, c, slot_block, slot_target, slot_count, weights, peer):
        block = donor(slot_block[c, peer])
        block = jnp.where(c < slot_count[0, peer], block, jnp.zeros_like(block))
        term = product(block, weights[peer, c])
        target = jnp.full((rows - comp, cells), slot_target[c, peer].astype(F32), F32)
        buf[r, c * rows : (c + 1) * rows, :] = jnp.concatenate([term, target], axis=0).astype(BF16)
        return term

    first = 4 + len(left_peers)
    second = first + 3 + len(send_peers)
    for load in loads[:first]:
        load.wait()
    for r in range(1, nl):
        peer = lax.rem(lvl + r, nl)
        for c in range(lcap):
            part += message(lsbuf, r, c, left_block, left_target, left_count, left_w, peer)
    for load in loads[first:second]:
        load.wait()
    for r in range(1, nd):
        peer = lax.rem(dev + r, nd)
        for c in range(cap):
            part += message(sbuf, r, c, send_block, send_target, send_count, send_w, peer)

    pl.semaphore_wait(barrier, len(near))
    if direct:
        for l in reversed(range(1, nl)):
            pl.semaphore_signal(entered, inc=1, device_id=peer_of(l, 0), device_id_type=MESH)

    sends = []

    def send(src, dst, s, d, who):
        copy = pltpu.make_async_remote_copy(
            src_ref=src, dst_ref=dst, send_sem=s, recv_sem=d, device_id=who, device_id_type=MESH
        )
        copy.start()
        sends.append(copy)
        return copy

    intras = [
        send(sbuf.at[r], rbuf.at[r], s_sem.at[r], r_sem.at[r], peer_of(0, r)) for r in range(1, nd)
    ]

    for load in loads[second:]:
        load.wait()
    acc = []
    for b in range(blocks):
        term = product(donor(own_src[0, b]), own_w[b])
        part += term
        acc.append(term)

    sums = jnp.sum(part, axis=1, keepdims=True)
    same = lax.broadcasted_iota(jnp.int32, (comp, cells), 0) == lax.broadcasted_iota(
        jnp.int32, (comp, cells), 1
    )
    row = jnp.sum(jnp.where(same, sums, 0.0), axis=0, keepdims=True)
    tbuf[...] = row

    if direct:
        pl.semaphore_wait(entered, nl - 1)
        tops = [
            send(tbuf, urecv.at[i], us_sem.at[i], ur_sem.at[i], peer_of(l, r))
            for i, (l, r) in enumerate(offsets)
        ]
    else:
        tots = [
            send(tbuf, trecv.at[r], ts_sem.at[r], tr_sem.at[r], peer_of(0, r))
            for r in range(1, nd)
        ]
    lefts = [
        send(lsbuf.at[r], lrbuf.at[r], ls_sem.at[r], lr_sem.at[r], peer_of(r, 0))
        for r in range(1, nl)
    ]
    if not direct:
        for r, copy in enumerate(tots, 1):
            copy.wait_recv()
            row += trecv[r]
        ubuf[...] = row
        tops = [
            send(ubuf, urecv.at[i], us_sem.at[i], ur_sem.at[i], peer_of(i + 1, 0))
            for i in range(nl - 1)
        ]

    def place(buf, r, slots):
        for c in range(slots):
            got = buf[r, c * rows : (c + 1) * rows, :].astype(F32)
            term = got[:comp]
            target = jnp.broadcast_to(got[comp : comp + 1], (comp, cells))
            for b in range(blocks):
                acc[b] = acc[b] + jnp.where(target == float(b), term, 0.0)

    for r, copy in enumerate(intras, 1):
        copy.wait_recv()
        place(rbuf, r, cap)
    for r, copy in enumerate(lefts, 1):
        copy.wait_recv()
        place(lrbuf, r, lcap)
    for b in range(blocks):
        out_ref[pl.ds(b, comp, stride=blocks), :] = acc[b]
    for copy in sends:
        copy.wait_send()
    for copy in tops:
        copy.wait_recv()
    terms = [row] + [urecv[i] for i in range(len(tops))]
    while len(terms) > 1:
        half = len(terms) // 2
        terms = [a + b for a, b in zip(terms[:half], terms[half:])] + terms[2 * half :]
    row = terms[0]
    tot_ref[...] = (row / (cells * blocks))[0, :comp]


def solution(mesh):
    nd = mesh.shape["dev"]
    nl = mesh.shape["level"]
    direct = nd * nl <= 64
    last = (nd if direct else 1) * nl

    def body(
        fields,
        own_src,
        own_weight,
        send_block,
        send_target,
        send_count,
        send_weight,
        left_block,
        left_target,
        left_count,
        left_weight,
    ):
        blocks, comp, cells = fields.shape[1:]
        cap = send_weight.shape[3]
        lcap = left_weight.shape[3]
        rows = -(-(comp + 1) // 16) * 16
        smem = functools.partial(pltpu.SMEM, dtype=jnp.int32)
        hbm = pl.BlockSpec(memory_space=pl.ANY)
        vmem = pl.BlockSpec(memory_space=pltpu.VMEM)
        dma = pltpu.SemaphoreType.DMA
        remapped, totals = pl.pallas_call(
            functools.partial(kernel, nd, nl, direct),
            out_shape=(
                pltpu.VMEM((comp * blocks, cells), F32),
                pltpu.VMEM((comp,), F32),
            ),
            in_specs=[hbm] * 11,
            out_specs=(vmem, vmem),
            scratch_shapes=[
                smem((1, blocks)),
                smem((cap, nd)),
                smem((cap, nd)),
                smem((1, nd)),
                smem((lcap, nl)),
                smem((lcap, nl)),
                smem((1, nl)),
                pltpu.VMEM((comp * blocks, cells), F32),
                pltpu.VMEM((blocks, cells, cells), BF16),
                pltpu.VMEM((nd, cap, cells, cells), BF16),
                pltpu.VMEM((nl, lcap, cells, cells), BF16),
                dma((9 + nd + nl,)),
                pltpu.VMEM((nd, cap * rows, cells), BF16),
                pltpu.VMEM((nd, cap * rows, cells), BF16),
                dma((nd,)),
                dma((nd,)),
                pltpu.VMEM((nl, lcap * rows, cells), BF16),
                pltpu.VMEM((nl, lcap * rows, cells), BF16),
                dma((nl,)),
                dma((nl,)),
                pltpu.VMEM((1, cells), F32),
                pltpu.VMEM((nd, 1, cells), F32),
                dma((nd,)),
                dma((nd,)),
                pltpu.VMEM((1, cells), F32),
                pltpu.VMEM((last, 1, cells), F32),
                dma((last,)),
                dma((last,)),
                pltpu.SemaphoreType.REGULAR,
            ],
            compiler_params=pltpu.CompilerParams(collective_id=0, has_side_effects=True),
        )(
            own_src,
            send_block[0, 0].T,
            send_target[0, 0].T,
            send_count[0],
            left_block[0, 0].T,
            left_target[0, 0].T,
            left_count[0],
            fields[0].transpose(1, 0, 2).reshape(comp * blocks, cells),
            own_weight[0],
            send_weight[0, 0],
            left_weight[0, 0],
        )
        remapped = remapped.reshape(comp, blocks, cells).transpose(1, 0, 2)
        return remapped[None], totals

    in_specs = (
        P("level", "dev", None, None),
        P("level", "dev"),
        P("level", "dev", None, None),
        P("level", "dev", None, None),
        P("level", "dev", None, None),
        P("level", "dev", None),
        P("level", "dev", None, None, None, None),
        P("level", "dev", None, None),
        P("level", "dev", None, None),
        P("level", "dev", None),
        P("level", "dev", None, None, None, None),
    )
    out_specs = (P("level", "dev", None, None), P())
    return jax.shard_map(body, mesh=mesh, in_specs=in_specs, out_specs=out_specs, check_vma=False)
```

```python
import functools

import jax
import jax.numpy as jnp
from jax import lax
from jax.experimental import pallas as pl
from jax.experimental.pallas import tpu as pltpu
from jax.sharding import PartitionSpec as P

MESH = pl.DeviceIdType.MESH
F32 = jnp.float32
BF16 = jnp.bfloat16


def kernel(
    nd,
    nl,
    direct,
    own_src_hbm,
    send_block_hbm,
    send_target_hbm,
    send_count_hbm,
    left_block_hbm,
    left_target_hbm,
    left_count_hbm,
    fields_hbm,
    own_hbm,
    send_hbm,
    left_hbm,
    out_ref,
    tot_ref,
    own_src,
    send_block,
    send_target,
    send_count,
    left_block,
    left_target,
    left_count,
    fields,
    own_w,
    send_w,
    left_w,
    load_sem,
    sbuf,
    rbuf,
    s_sem,
    r_sem,
    lsbuf,
    lrbuf,
    ls_sem,
    lr_sem,
    tbuf,
    trecv,
    ts_sem,
    tr_sem,
    ubuf,
    urecv,
    us_sem,
    ur_sem,
):
    dev = lax.axis_index("dev")
    lvl = lax.axis_index("level")
    blocks, cells = own_w.shape[:2]
    comp = fields.shape[0] // blocks
    cap = send_w.shape[1]
    lcap = left_w.shape[1]
    rows = sbuf.shape[1] // cap

    barrier = pltpu.get_barrier_semaphore()
    left_peers = [lax.rem(lvl + r, nl) for r in range(1, nl)]
    send_peers = [lax.rem(dev + r, nd) for r in range(1, nd)]
    pairs = (
        (left_block_hbm, left_block),
        (left_target_hbm, left_target),
        (left_count_hbm, left_count),
        (fields_hbm, fields),
        *[(left_hbm.at[p], left_w.at[p]) for p in left_peers],
        (send_block_hbm, send_block),
        (send_target_hbm, send_target),
        (send_count_hbm, send_count),
        *[(send_hbm.at[p], send_w.at[p]) for p in send_peers],
        (own_src_hbm, own_src),
        (own_hbm, own_w),
    )
    loads = [
        pltpu.make_async_copy(src, dst, load_sem.at[i]) for i, (src, dst) in enumerate(pairs)
    ]
    for load in loads:
        load.start()

    def peer_of(l, r):
        return {"level": lax.rem(lvl + l, nl), "dev": lax.rem(dev + r, nd)}

    offsets = [
        (l, r)
        for l in reversed(range(nl))
        for r in reversed(range(nd))
        if (l or r) and (direct or not (l and r))
    ]
    for l, r in offsets:
        pl.semaphore_signal(barrier, inc=1, device_id=peer_of(l, r), device_id_type=MESH)

    part = jnp.zeros((comp, cells), F32)

    def donor(index):
        return fields[pl.ds(index, comp, stride=blocks), :]

    def product(block, weight):
        return jnp.dot(block.astype(BF16), weight, preferred_element_type=F32)

    def message(buf, r, c, slot_block, slot_target, slot_count, weights, peer):
        block = donor(slot_block[c, peer])
        block = jnp.where(c < slot_count[0, peer], block, jnp.zeros_like(block))
        term = product(block, weights[peer, c])
        target = jnp.full((rows - comp, cells), slot_target[c, peer].astype(F32), F32)
        buf[r, c * rows : (c + 1) * rows, :] = jnp.concatenate([term, target], axis=0).astype(BF16)
        return term

    first = 4 + len(left_peers)
    second = first + 3 + len(send_peers)
    for load in loads[:first]:
        load.wait()
    for r in range(1, nl):
        peer = lax.rem(lvl + r, nl)
        for c in range(lcap):
            part += message(lsbuf, r, c, left_block, left_target, left_count, left_w, peer)
    for load in loads[first:second]:
        load.wait()
    for r in range(1, nd):
        peer = lax.rem(dev + r, nd)
        for c in range(cap):
            part += message(sbuf, r, c, send_block, send_target, send_count, send_w, peer)

    for load in loads[second:]:
        load.wait()
    acc = []
    for b in range(blocks):
        term = product(donor(own_src[0, b]), own_w[b])
        part += term
        acc.append(term)

    sums = jnp.sum(part, axis=1, keepdims=True)
    same = lax.broadcasted_iota(jnp.int32, (comp, cells), 0) == lax.broadcasted_iota(
        jnp.int32, (comp, cells), 1
    )
    row = jnp.sum(jnp.where(same, sums, 0.0), axis=0, keepdims=True)
    tbuf[...] = row

    pl.semaphore_wait(barrier, len(offsets))

    sends = []

    def send(src, dst, s, d, who):
        copy = pltpu.make_async_remote_copy(
            src_ref=src, dst_ref=dst, send_sem=s, recv_sem=d, device_id=who, device_id_type=MESH
        )
        copy.start()
        sends.append(copy)
        return copy

    intras = [
        send(sbuf.at[r], rbuf.at[r], s_sem.at[r], r_sem.at[r], peer_of(0, r)) for r in range(1, nd)
    ]
    if direct:
        tops = [
            send(tbuf, urecv.at[i], us_sem.at[i], ur_sem.at[i], peer_of(l, r))
            for i, (l, r) in enumerate(offsets)
        ]
    else:
        tots = [
            send(tbuf, trecv.at[r], ts_sem.at[r], tr_sem.at[r], peer_of(0, r))
            for r in range(1, nd)
        ]
    lefts = [
        send(lsbuf.at[r], lrbuf.at[r], ls_sem.at[r], lr_sem.at[r], peer_of(r, 0))
        for r in range(1, nl)
    ]
    if not direct:
        for r, copy in enumerate(tots, 1):
            copy.wait_recv()
            row += trecv[r]
        ubuf[...] = row
        tops = [
            send(ubuf, urecv.at[i], us_sem.at[i], ur_sem.at[i], peer_of(i + 1, 0))
            for i in range(nl - 1)
        ]

    def place(buf, r, slots):
        for c in range(slots):
            got = buf[r, c * rows : (c + 1) * rows, :].astype(F32)
            term = got[:comp]
            target = jnp.broadcast_to(got[comp : comp + 1], (comp, cells))
            for b in range(blocks):
                acc[b] = acc[b] + jnp.where(target == float(b), term, 0.0)

    for r, copy in enumerate(intras, 1):
        copy.wait_recv()
        place(rbuf, r, cap)
    for r, copy in enumerate(lefts, 1):
        copy.wait_recv()
        place(lrbuf, r, lcap)
    for b in range(blocks):
        out_ref[pl.ds(b, comp, stride=blocks), :] = acc[b]
    for copy in sends:
        copy.wait_send()
    for copy in tops:
        copy.wait_recv()
    terms = [row] + [urecv[i] for i in range(len(tops))]
    while len(terms) > 1:
        half = len(terms) // 2
        terms = [a + b for a, b in zip(terms[:half], terms[half:])] + terms[2 * half :]
    row = terms[0]
    tot_ref[...] = (row / (cells * blocks))[0, :comp]


def solution(mesh):
    nd = mesh.shape["dev"]
    nl = mesh.shape["level"]
    direct = nd * nl <= 64
    last = (nd if direct else 1) * nl

    def body(
        fields,
        own_src,
        own_weight,
        send_block,
        send_target,
        send_count,
        send_weight,
        left_block,
        left_target,
        left_count,
        left_weight,
    ):
        blocks, comp, cells = fields.shape[1:]
        cap = send_weight.shape[3]
        lcap = left_weight.shape[3]
        rows = -(-(comp + 1) // 16) * 16
        smem = functools.partial(pltpu.SMEM, dtype=jnp.int32)
        hbm = pl.BlockSpec(memory_space=pl.ANY)
        vmem = pl.BlockSpec(memory_space=pltpu.VMEM)
        dma = pltpu.SemaphoreType.DMA
        remapped, totals = pl.pallas_call(
            functools.partial(kernel, nd, nl, direct),
            out_shape=(
                pltpu.VMEM((comp * blocks, cells), F32),
                pltpu.VMEM((comp,), F32),
            ),
            in_specs=[hbm] * 11,
            out_specs=(vmem, vmem),
            scratch_shapes=[
                smem((1, blocks)),
                smem((cap, nd)),
                smem((cap, nd)),
                smem((1, nd)),
                smem((lcap, nl)),
                smem((lcap, nl)),
                smem((1, nl)),
                pltpu.VMEM((comp * blocks, cells), F32),
                pltpu.VMEM((blocks, cells, cells), BF16),
                pltpu.VMEM((nd, cap, cells, cells), BF16),
                pltpu.VMEM((nl, lcap, cells, cells), BF16),
                dma((9 + nd + nl,)),
                pltpu.VMEM((nd, cap * rows, cells), BF16),
                pltpu.VMEM((nd, cap * rows, cells), BF16),
                dma((nd,)),
                dma((nd,)),
                pltpu.VMEM((nl, lcap * rows, cells), BF16),
                pltpu.VMEM((nl, lcap * rows, cells), BF16),
                dma((nl,)),
                dma((nl,)),
                pltpu.VMEM((1, cells), F32),
                pltpu.VMEM((nd, 1, cells), F32),
                dma((nd,)),
                dma((nd,)),
                pltpu.VMEM((1, cells), F32),
                pltpu.VMEM((last, 1, cells), F32),
                dma((last,)),
                dma((last,)),
            ],
            compiler_params=pltpu.CompilerParams(collective_id=0, has_side_effects=True),
        )(
            own_src,
            send_block[0, 0].T,
            send_target[0, 0].T,
            send_count[0],
            left_block[0, 0].T,
            left_target[0, 0].T,
            left_count[0],
            fields[0].transpose(1, 0, 2).reshape(comp * blocks, cells),
            own_weight[0],
            send_weight[0, 0],
            left_weight[0, 0],
        )
        remapped = remapped.reshape(comp, blocks, cells).transpose(1, 0, 2)
        return remapped[None], totals

    in_specs = (
        P("level", "dev", None, None),
        P("level", "dev"),
        P("level", "dev", None, None),
        P("level", "dev", None, None),
        P("level", "dev", None, None),
        P("level", "dev", None),
        P("level", "dev", None, None, None, None),
        P("level", "dev", None, None),
        P("level", "dev", None, None),
        P("level", "dev", None),
        P("level", "dev", None, None, None, None),
    )
    out_specs = (P("level", "dev", None, None), P())
    return jax.shard_map(body, mesh=mesh, in_specs=in_specs, out_specs=out_specs, check_vma=False)
```
